32 devices in a mesh: win: 2 (over y), dx: 4 (over z), dy: 2 (over x), dz: 2 (over core).
Axes of the slice: x: 2, y: 2, z: 4, core: 2. Of those that a mesh axis runs over, the one named last changes fastest.
Arguments:
- fraction: float32 [3, 8, 2, 2, 768], P(None, ('win', 'dx'), 'dy', 'dz'), parts along dimension 1, may hold values from 0 to 1
- atom_type: int32 [8, 2, 2, 768], P(('win', 'dx'), 'dy', 'dz'), parts along dimension 0, may hold values from 0 to 31
- perturbed: int32 [8, 2, 2, 768], P(('win', 'dx'), 'dy', 'dz'), parts along dimension 0, may hold values from 0 to 1
- leaving: int32 [8, 2, 2, 2, 16], P(('win', 'dx'), 'dy', 'dz'), parts along dimension 0, may hold values from 0 to 767, as said below
- neighbours: int32 [8, 2, 2, 6, 16], P(('win', 'dx'), 'dy', 'dz'), parts along dimension 0, may hold values from 0 to 161, as said below
- counts: int32 [8, 2, 2, 6], P(('win', 'dx'), 'dy', 'dz'), parts along dimension 0, may hold values from 1 to 16, as said below
- sigma_table: float32 [32], replicated, may hold values from 0.8 to 1.2
- depth_table: float32 [32], replicated, may hold values from 0.002 to 0.03
- charge_table: float32 [32], replicated, may hold values from -1 to 1
- domain_edge: float32 [3], replicated, may hold values from 1 to 1.12
- coupling: float32 [2], P('win'), parts along dimension 0, may hold values from 0.1 to 0.9
Outputs:
- forces: float32 [3, 8, 2, 2, 768], P(None, ('win', 'dx'), 'dy', 'dz'), parts along dimension 1
- energy: float32 [2], P('win'), parts along dimension 0
- dhdl: float32 [2], P('win'), parts along dimension 0
The draws below stay inside these ranges and needn't reach their ends.
There are 2 independent parts, one for each index of `win`. The reference program is written for one: setup_inputs(seed, part) draws one part's arguments, and reference() takes and returns one part's arrays. A program takes and returns all parts, laid end to end along the dimension named above; an argument that names none is the same for every part. Nothing has to cross between parts.
Inputs may be any that keep to these rules, and one draw needn't show every extreme that they name: `leaving`: each domain lists 2 * 16 distinct slots: the first 16 leave toward the next domain, the last 16 toward the previous one. `neighbours`: each list holds 16 distinct ghost block numbers; entries at or past the block's count are valid numbers and are not used. `counts`: some block lists exactly 16 blocks in every draw.
All inputs are finite; a program needn't handle non-finite values.
Results may differ from the reference program's by a relative error of at most 0.0003.
Values sent between devices are 32-bit elements; how exact they have to be, the bound alone decides.
A program may use at most 64 MiB of HBM per device.

```python
import math
import jax
import jax.numpy as jnp
from jax import lax

ATOMS_DEV = 768
NB = 16
MIG = 16
NTYPES = 32
NATOMS = 12288
N_DX = 4
N_DY = 2
N_DZ = 2


def draw_perturbed(key, part):
    shape = (N_DX, N_DY, N_DZ, ATOMS_DEV)
    position_x = jnp.arange(N_DX, dtype=jnp.int32)[:, None, None, None]
    threshold = 10 + 20 * position_x // max(N_DX - 1, 1)
    values = jax.random.randint(key, shape, 0, 100, dtype=jnp.int32)
    return (values < threshold).astype(jnp.int32)


def draw_leaving(key, part):
    shape = (N_DX, N_DY, N_DZ, ATOMS_DEV)
    scores = jax.random.randint(key, shape, 0, 2 ** 16, dtype=jnp.int32) * ATOMS_DEV + jnp.arange(ATOMS_DEV, dtype=jnp.int32)
    order = jnp.argsort(scores, axis=-1, stable=True).astype(jnp.int32)
    return order[..., :2 * MIG].reshape(N_DX, N_DY, N_DZ, 2, MIG)


def draw_neighbours(key, part):
    ghost_blocks = 27 * (ATOMS_DEV // 128)
    shape = (N_DX, N_DY, N_DZ, ATOMS_DEV // 128, ghost_blocks)
    scores = jax.random.randint(key, shape, 0, 2 ** 16, dtype=jnp.int32) * ghost_blocks + jnp.arange(ghost_blocks, dtype=jnp.int32)
    order = jnp.argsort(scores, axis=-1, stable=True).astype(jnp.int32)
    return order[..., :NB]


def draw_counts(key, part):
    shape = (N_DX, N_DY, N_DZ, ATOMS_DEV // 128)
    values = jax.random.randint(key, shape, 1, NB + 1, dtype=jnp.int32)
    return values.at[0, 0, 0, 0].set(NB)


def touch_ends(array, key, smallest, top_value):
    longest = array.shape.index(max(array.shape))
    spots = []
    for shift in (0, 1):
        where = [jax.random.randint(jax.random.fold_in(key, axis), (), 0, length) for axis, length in enumerate(array.shape)]
        where[longest] = (where[longest] + shift) % array.shape[longest]
        spots.append(tuple(where))
    return array.at[spots[0]].set(smallest).at[spots[1]].set(top_value)


def levels(own_key, extent, cuts, least, high):
    factor_of, own = 1.0, jax.random.fold_in(own_key, 6)
    for dim, parts in cuts:
        steps = jnp.exp(jax.random.uniform(jax.random.fold_in(own, dim), (parts,), jnp.float32, least / len(cuts), high / len(cuts)))
        factor_of = factor_of * jnp.repeat(steps, extent[dim] // parts).reshape([-1 if axis == dim else 1 for axis in range(len(extent))])
    return factor_of


def setup_inputs(seed: int = 0, part: int = 0) -> dict:
    seeds = jax.random.split(jax.random.key(seed), 12)
    part_splits = jax.random.split(jax.random.fold_in(seeds[11], part), 12)
    fraction = jnp.clip(1.0 * jax.random.uniform(part_splits[0], (3, N_DX, N_DY, N_DZ, ATOMS_DEV), jnp.float32) ** levels(part_splits[0], (3, N_DX, N_DY, N_DZ, ATOMS_DEV), ((1, 4), (2, 2), (3, 2)), -0.2, 0.2), 0.0, 1.0)
    atom_type = touch_ends(jax.random.randint(part_splits[1], (N_DX, N_DY, N_DZ, ATOMS_DEV), 0, NTYPES), jax.random.fold_in(part_splits[1], 1), 0, NTYPES - 1).astype(jnp.int32)
    perturbed = draw_perturbed(jax.random.fold_in(jax.random.fold_in(seeds[11], part), 71), part)
    leaving = draw_leaving(jax.random.fold_in(jax.random.fold_in(seeds[11], part), 71), part)
    neighbours = draw_neighbours(jax.random.fold_in(jax.random.fold_in(seeds[11], part), 71), part)
    counts = draw_counts(jax.random.fold_in(jax.random.fold_in(seeds[11], part), 71), part)
    sigma_table = jnp.clip(jnp.exp(jax.random.uniform(seeds[6], (NTYPES,), jnp.float32, math.log(0.8), math.log(1.2))), 0.8, 1.2)
    depth_table = jnp.clip(jnp.exp(jax.random.uniform(seeds[7], (NTYPES,), jnp.float32, math.log(0.002), math.log(0.03))), 0.002, 0.03)
    charge_table = jnp.clip(jax.random.uniform(seeds[8], (NTYPES,), jnp.float32, -1.0, 1.0), -1.0, 1.0)
    domain_edge = jnp.clip(jax.random.uniform(seeds[9], (3,), jnp.float32, 1.0, 1.12), 1.0, 1.12)
    coupling = jnp.clip(jax.random.uniform(part_splits[10], (1,), jnp.float32, 0.1, 0.9), 0.1, 0.9)
    return {"fraction": fraction, "atom_type": atom_type, "perturbed": perturbed, "leaving": leaving, "neighbours": neighbours, "counts": counts, "sigma_table": sigma_table, "depth_table": depth_table, "charge_table": charge_table, "domain_edge": domain_edge, "coupling": coupling}


soft_base = 0.3
soft_alpha = 0.5
charge_base = 0.3
charge_alpha = 0.5
coulomb = 0.1

def lookup(table_row, type_ids):
    onehot = type_ids[None, :] == jnp.arange(table_row.shape[0], dtype=jnp.int32)[:, None]
    return lax.optimization_barrier(jnp.sum(jnp.where(onehot, table_row[:, None], jnp.float32(0.0)), axis=0))

def pair_block(own_block, other_blocks, live_pairs, coupling_value):
    separation = own_block[0:3][None, :, :, None] - other_blocks[:, 0:3][:, :, None, :]
    radius_sq = lax.optimization_barrier(jnp.sum(separation * separation, axis=1))
    sigma_pair = 0.5 * (own_block[3][None, :, None] + other_blocks[:, 3][:, None, :])
    depth_pair = jnp.sqrt(own_block[4][None, :, None] * other_blocks[:, 4][:, None, :])
    charges = own_block[5][None, :, None] * other_blocks[:, 5][:, None, :]
    flagged = jnp.maximum(own_block[6][None, :, None], other_blocks[:, 6][:, None, :])
    scaled = coupling_value * flagged
    sigma_two = sigma_pair * sigma_pair
    sigma_six = sigma_two * sigma_two * sigma_two
    soft_six = sigma_six * (soft_base + soft_alpha * scaled) + radius_sq * radius_sq * radius_sq
    soft_two = charge_base + charge_alpha * scaled + radius_sq
    inverse_six = 1.0 / soft_six
    energy_lj = 4.0 * depth_pair * (sigma_six * sigma_six * inverse_six * inverse_six - sigma_six * inverse_six)
    grad_six = 4.0 * depth_pair * (sigma_six * inverse_six * inverse_six - 2.0 * sigma_six * sigma_six * inverse_six * inverse_six * inverse_six)
    energy_coul = coulomb * charges * lax.rsqrt(soft_two)
    grad_two = -0.5 * energy_coul / soft_two
    weight = 1.0 - scaled
    total_pair = energy_lj + energy_coul
    pair_energy = jnp.sum(weight * total_pair * live_pairs)
    pair_dhdl = jnp.sum(flagged * (-total_pair + weight * (grad_six * sigma_six * soft_alpha + grad_two * charge_alpha)) * live_pairs)
    force_scale = -weight * (6.0 * radius_sq * radius_sq * grad_six + 2.0 * grad_two) * live_pairs
    forces = lax.optimization_barrier(jnp.sum(force_scale[:, None] * separation, axis=(0, 3)))
    return (forces, pair_energy, pair_dhdl)

def block_terms(ghost_rows, listed_blocks, list_count, block_id, block_total, coupling_value):
    centre = 13 * block_total + block_id
    own_block = lax.dynamic_index_in_dim(ghost_rows, centre, 0, keepdims=False)
    other_blocks = jnp.take(ghost_rows, listed_blocks, axis=0)
    valid_slot = (jnp.arange(listed_blocks.shape[0], dtype=jnp.int32) < list_count).astype(jnp.float32)
    is_self = (listed_blocks == centre).astype(jnp.float32)[:, None, None] * jnp.eye(128, dtype=jnp.float32)[None]
    live_pairs = valid_slot[:, None, None] * (1.0 - is_self)
    return pair_block(own_block, other_blocks, live_pairs, coupling_value)

def reference(fraction, atom_type, perturbed, leaving, neighbours, counts, sigma_table, depth_table, charge_table, domain_edge, coupling):
    domains = N_DX * N_DY * N_DZ
    block_total = ATOMS_DEV // 128
    spacing = float(ATOMS_DEV) ** (1.0 / 3.0)
    type_ids = atom_type.reshape(-1)
    payload = jnp.concatenate([fraction.reshape(3, domains, ATOMS_DEV), lookup(sigma_table, type_ids).reshape(1, domains, ATOMS_DEV), lookup(depth_table, type_ids).reshape(1, domains, ATOMS_DEV), lookup(charge_table, type_ids).reshape(1, domains, ATOMS_DEV), perturbed.reshape(1, domains, ATOMS_DEV).astype(jnp.float32)], axis=0)
    leave_slots = leaving.reshape(domains, 2, MIG)
    upward = jnp.take_along_axis(payload, leave_slots[None, :, 0, :], axis=2)
    downward = jnp.take_along_axis(payload, leave_slots[None, :, 1, :], axis=2)
    shift_x = jnp.zeros((7, 1, 1), jnp.float32).at[0].set(1.0)
    from_below = jnp.roll(upward.reshape(7, N_DX, N_DY * N_DZ, MIG), 1, axis=1).reshape(7, domains, MIG) - shift_x
    from_above = jnp.roll(downward.reshape(7, N_DX, N_DY * N_DZ, MIG), -1, axis=1).reshape(7, domains, MIG) + shift_x

    def place(block_rows, down_slots, up_slots, lower_rows, upper_rows):
        return block_rows.at[:, down_slots].set(lower_rows).at[:, up_slots].set(upper_rows)
    moved = jax.vmap(place, in_axes=(1, 0, 0, 1, 1), out_axes=1)(payload, leave_slots[:, 1], leave_slots[:, 0], from_below, from_above)
    moved_grid = moved.reshape(7, N_DX, N_DY, N_DZ, ATOMS_DEV)
    list_flat = neighbours.reshape(domains, block_total, NB)
    count_flat = counts.reshape(domains, block_total)
    coupling_value = coupling[0]

    def one_domain(flat_id):
        index_x = flat_id // (N_DY * N_DZ)
        index_y = flat_id // N_DZ % N_DY
        index_z = flat_id % N_DZ
        pieces = []
        for step_x in range(3):
            for step_y in range(3):
                for step_z in range(3):
                    neighbour_rows = moved_grid[:, (index_x + step_x - 1) % N_DX, (index_y + step_y - 1) % N_DY, (index_z + step_z - 1) % N_DZ]
                    position = jnp.stack([(neighbour_rows[0] + jnp.float32(step_x - 1)) * domain_edge[0] * spacing, (neighbour_rows[1] + jnp.float32(step_y - 1)) * domain_edge[1] * spacing, (neighbour_rows[2] + jnp.float32(step_z - 1)) * domain_edge[2] * spacing], axis=0)
                    pieces.append(jnp.concatenate([position, neighbour_rows[3:]], axis=0))
        ghost_rows = jnp.stack(pieces, 0).reshape(27, 7, block_total, 128).transpose(0, 2, 1, 3).reshape(27 * block_total, 7, 128)
        listed = list_flat[flat_id]
        listed_count = count_flat[flat_id]

        def one_block(block_id):
            return block_terms(ghost_rows, listed[block_id], listed_count[block_id], block_id, block_total, coupling_value)
        forces, energies, dhdls = lax.map(one_block, jnp.arange(block_total, dtype=jnp.int32))
        return (forces.transpose(1, 0, 2).reshape(3, ATOMS_DEV), jnp.sum(energies), jnp.sum(dhdls))
    forces, energies, dhdls = lax.map(one_domain, jnp.arange(domains, dtype=jnp.int32))
    forces = forces.transpose(1, 0, 2).reshape(3, N_DX, N_DY, N_DZ, ATOMS_DEV)
    energy = (0.5 * jnp.sum(energies) / jnp.float32(NATOMS)).reshape(1)
    dhdl = (0.5 * jnp.sum(dhdls) / jnp.float32(NATOMS)).reshape(1)
    return (forces, energy, dhdl)
```

```python
import jax
import jax.numpy as jnp
from jax import lax
from jax.experimental import pallas as pl
from jax.experimental.pallas import tpu as pltpu
from jax.sharding import PartitionSpec as P

soft_base = 0.3
soft_alpha = 0.5
charge_base = 0.3
charge_alpha = 0.5
coulomb = 0.1
LANES = 128
MESH = pl.DeviceIdType.MESH
HIGHEST = lax.Precision.HIGHEST


def steps_of(count):
    return {1: (0,), 2: (0, 1)}.get(count, (-1, 0, 1))


def slot_step(step, count):
    if count == 1:
        return step * 0
    if count == 2:
        return step * step
    return step + 1


def halo_kernel(
    sizes,
    sigma_ref,
    depth_ref,
    charge_ref,
    edge_ref,
    fraction_ref,
    type_ref,
    flag_ref,
    leaving_ref,
    ghost_ref,
    outgoing,
    incoming,
    mig_send,
    mig_recv,
    send_sem,
    recv_sem,
):
    nx, ny, nz = sizes
    atoms = fraction_ref.shape[-1]
    spacing = float(atoms) ** (1.0 / 3.0)
    me = (lax.axis_index("dx"), lax.axis_index("dy"), lax.axis_index("dz"))

    def device(step):
        return {
            name: lax.rem(place + by + count, count)
            for name, place, by, count in zip(("dx", "dy", "dz"), me, step, sizes)
        }

    offsets = [(a, b, c) for a in steps_of(nx) for b in steps_of(ny) for c in steps_of(nz)]
    others = [o for o in offsets if any(o)]

    def slot(o):
        return (
            slot_step(o[0], nx) * len(steps_of(ny)) + slot_step(o[1], ny)
        ) * len(steps_of(nz)) + slot_step(o[2], nz)

    barrier = pltpu.get_barrier_semaphore()
    for o in others:
        pl.semaphore_signal(
            barrier, inc=1, device_id=device(tuple(-x for x in o)), device_id_type=MESH
        )

    own = ghost_ref.at[slot((0, 0, 0))]
    types = type_ref[0, 0]
    sigma = jnp.zeros((1, atoms), jnp.float32)
    depth = jnp.zeros((1, atoms), jnp.float32)
    charge = jnp.zeros((1, atoms), jnp.float32)
    for k in range(sigma_ref.shape[0]):
        hit = types == k
        sigma = jnp.where(hit, sigma_ref[k], sigma)
        depth = jnp.where(hit, depth_ref[k], depth)
        charge = jnp.where(hit, charge_ref[k], charge)
    edge = [edge_ref[k] * spacing for k in range(3)]
    rows = [fraction_ref[k, 0, 0] * edge[k] for k in range(3)]
    flag = flag_ref[0, 0].astype(jnp.float32)
    rows += [sigma * 0.5, jnp.sqrt(depth) * 2.0, charge, flag, flag * 0.0]
    payload = jnp.concatenate(rows, axis=0)
    leave = leaving_ref[0, 0, 0]
    mig = leave.shape[1]
    place = lax.broadcasted_iota(jnp.int32, (atoms, mig), 0)
    up_hot = (place == leave[0:1]).astype(jnp.float32)
    down_hot = (place == leave[1:2]).astype(jnp.float32)
    first = lax.broadcasted_iota(jnp.int32, (8, mig), 0) == 0
    shift = jnp.where(first, edge[0], 0.0)
    outgoing[0] = jnp.dot(payload, up_hot, precision=HIGHEST) - shift
    outgoing[1] = jnp.dot(payload, down_hot, precision=HIGHEST) + shift
    contract = (((1,), (1,)), ((), ()))
    ones = jnp.ones((8, mig), jnp.float32)
    gone = lax.dot_general(ones, up_hot + down_hot, contract, precision=HIGHEST)
    kept = jnp.where(gone > 0.5, 0.0, payload)

    pl.semaphore_wait(barrier, len(others))
    moves = []
    for side, by in ((0, 1), (1, -1)):
        move = pltpu.make_async_remote_copy(
            src_ref=outgoing.at[side],
            dst_ref=incoming.at[side],
            send_sem=mig_send.at[side],
            recv_sem=mig_recv.at[side],
            device_id=device((by, 0, 0)),
            device_id_type=MESH,
        )
        move.start()
        moves.append(move)
    for move in moves:
        move.wait()
    from_below = lax.dot_general(incoming[0], down_hot, contract, precision=HIGHEST)
    from_above = lax.dot_general(incoming[1], up_hot, contract, precision=HIGHEST)
    own[...] = kept + from_below + from_above
    copies = []
    for k, o in enumerate(sorted(others, key=lambda o: -sum(map(abs, o)))):
        copy = pltpu.make_async_remote_copy(
            src_ref=own,
            dst_ref=ghost_ref.at[slot(o)],
            send_sem=send_sem.at[k],
            recv_sem=recv_sem.at[k],
            device_id=device(tuple(-x for x in o)),
            device_id_type=MESH,
        )
        copy.start()
        copies.append(copy)
    for copy in copies:
        copy.wait()


def pair_kernel(
    sizes,
    listed_ref,
    count_ref,
    edge_ref,
    coupling_ref,
    ghost_ref,
    force_ref,
    sums_ref,
    own_cols,
    force_acc,
):
    nx, ny, nz = sizes
    atoms = ghost_ref.shape[-1]
    blocks = atoms // LANES
    spacing = float(atoms) ** (1.0 / 3.0)
    edge = [edge_ref[k] * spacing for k in range(3)]
    lam = coupling_ref[0]
    own_slot = (slot_step(0, nx) * len(steps_of(ny)) + slot_step(0, ny)) * len(
        steps_of(nz)
    ) + slot_step(0, nz)
    ones = jnp.ones((8, LANES), jnp.float32)
    for k in range(3):
        sums_ref[k] = jnp.zeros((8, LANES), jnp.float32)

    def derived(flag):
        scaled = lam * flag
        return soft_base + soft_alpha * scaled, 1.0 - scaled

    @pl.loop(0, blocks)
    def _(q):
        base = pl.multiple_of(q * LANES, LANES)
        cols = ghost_ref[own_slot, :, pl.ds(base, LANES)].T
        for r in range(7):
            own_cols[r] = jnp.broadcast_to(cols[:, r : r + 1], (LANES, LANES))
        own_cols[5] = own_cols[5] * coulomb
        soft, weight = derived(own_cols[6])
        own_cols[7] = soft
        own_cols[8] = weight
        for k in range(3):
            force_acc[k] = jnp.zeros((LANES, LANES), jnp.float32)

        @pl.loop(0, count_ref[0, 0, 0, q])
        def _(e):
            listed = listed_ref[0, 0, 0, q, e]
            image = lax.div(listed, blocks)
            start = pl.multiple_of(lax.rem(listed, blocks) * LANES, LANES)
            a = lax.div(image, 9) - 1
            b = lax.rem(lax.div(image, 3), 3) - 1
            c = lax.rem(image, 3) - 1
            where_from = (
                slot_step(a, nx) * len(steps_of(ny)) + slot_step(b, ny)
            ) * len(steps_of(nz)) + slot_step(c, nz)
            rows = []
            for r in range(7):
                row = ghost_ref[where_from, pl.ds(r, 1), pl.ds(start, LANES)]
                if r < 3:
                    row = row + (a, b, c)[r].astype(jnp.float32) * edge[r]
                rows.append(jnp.broadcast_to(row, (8, LANES)))
            xj, yj, zj, hj, ej, qj, pj = rows
            aj, wj = derived(pj)

            def terms(masked):
                tot = jnp.zeros((8, LANES), jnp.float32)
                tot_p = jnp.zeros((8, LANES), jnp.float32)
                tot_k = jnp.zeros((8, LANES), jnp.float32)
                for g in range(LANES // 8):
                    at = pl.ds(g * 8, 8)
                    dx = own_cols[0, at] - xj
                    dy = own_cols[1, at] - yj
                    dz = own_cols[2, at] - zj
                    r2 = dx * dx + dy * dy + dz * dz
                    sig = own_cols[3, at] + hj
                    s2 = sig * sig
                    s6 = s2 * s2 * s2
                    eps4 = own_cols[4, at] * ej
                    qq = own_cols[5, at] * qj
                    if masked:
                        diag = (
                            lax.broadcasted_iota(jnp.int32, (8, LANES), 0) + g * 8
                            == lax.broadcasted_iota(jnp.int32, (8, LANES), 1)
                        )
                        eps4 = jnp.where(diag, 0.0, eps4)
                        qq = jnp.where(diag, 0.0, qq)
                    p = jnp.maximum(own_cols[6, at], pj)
                    soft = jnp.maximum(own_cols[7, at], aj)
                    weight = jnp.minimum(own_cols[8, at], wj)
                    r4 = r2 * r2
                    soft6 = s6 * soft + r4 * r2
                    inv = 1.0 / soft6
                    u = lax.rsqrt(soft + r2)
                    ec = qq * u
                    half = (0.5 * ec) * (u * u)
                    t = s6 * inv
                    et = eps4 * t
                    tm = t - 1.0
                    v = et * tm + ec
                    m = et * (t + tm)
                    kk = m * t + half
                    fs = weight * (3.0 * (m * (r4 * inv)) + half)
                    tot = tot + v
                    tot_p = tot_p + p * v
                    tot_k = tot_k + p * kk
                    force_acc[0, at] += fs * dx
                    force_acc[1, at] += fs * dy
                    force_acc[2, at] += fs * dz
                sums_ref[0] += tot
                sums_ref[1] += tot_p
                sums_ref[2] += tot_k

            is_self = listed == 13 * blocks + q

            @pl.when(is_self)
            def _():
                terms(True)

            @pl.when(jnp.logical_not(is_self))
            def _():
                terms(False)

        for k in range(3):
            total = lax.dot_general(
                ones, force_acc[k], (((1,), (1,)), ((), ())), precision=HIGHEST
            )
            force_ref[k, 0, 0, :, pl.ds(base, LANES)] = 2.0 * total[0:1]


def sum_kernel(sizes, atoms, coupling_ref, sums_ref, energy_ref, dhdl_ref, tile, gathered, send_sem, recv_sem):
    nx, ny, nz = sizes
    total = nx * ny * nz
    me = (lax.axis_index("dx") * ny + lax.axis_index("dy")) * nz + lax.axis_index("dz")

    def device(k):
        return {"dx": k // (ny * nz), "dy": k // nz % ny, "dz": k % nz}

    barrier = pltpu.get_barrier_semaphore()

    @pl.loop(1, total)
    def _(by):
        pl.semaphore_signal(
            barrier, inc=1, device_id=device(lax.rem(me + by, total)), device_id_type=MESH
        )

    rows = [jnp.sum(sums_ref[k], axis=0, keepdims=True) for k in range(3)]
    rows.append(jnp.zeros((5, LANES), jnp.float32))
    tile[...] = jnp.concatenate(rows, axis=0)
    gathered[me] = tile[...]
    pl.semaphore_wait(barrier, total - 1)

    def copy(by):
        return pltpu.make_async_remote_copy(
            src_ref=tile,
            dst_ref=gathered.at[me],
            send_sem=send_sem.at[by],
            recv_sem=recv_sem.at[by],
            device_id=device(lax.rem(me + by, total)),
            device_id_type=MESH,
        )

    @pl.loop(1, total)
    def _(by):
        copy(by).start()

    @pl.loop(1, total)
    def _(by):
        copy(by).wait()

    summed = jnp.sum(gathered[...], axis=0)
    whole = [jnp.sum(summed[k : k + 1]) for k in range(3)]
    lam = coupling_ref[0]
    scale = 0.5 / float(atoms * total)
    energy_ref[0] = scale * (whole[0] - lam * whole[1])
    dhdl_ref[0] = -scale * (whole[1] + (0.5 * (1.0 - lam)) * whole[2])


def on_device(sizes, fraction, atom_type, perturbed, leaving, neighbours, counts,
              sigma_table, depth_table, charge_table, domain_edge, coupling):
    nx, ny, nz = sizes
    atoms = fraction.shape[-1]
    mig = leaving.shape[-1]
    slots = len(steps_of(nx)) * len(steps_of(ny)) * len(steps_of(nz))
    smem = pl.BlockSpec(memory_space=pltpu.SMEM)
    vmem = pl.BlockSpec(memory_space=pltpu.VMEM)
    f32 = jnp.float32

    def bound(kernel, *values):
        return lambda *refs: kernel(*values, *refs)

    ghosts = pl.pallas_call(
        bound(halo_kernel, sizes),
        name="halo",
        out_shape=jax.ShapeDtypeStruct((slots, 8, atoms), f32),
        in_specs=[smem] * 4 + [vmem] * 4,
        out_specs=vmem,
        scratch_shapes=[
            pltpu.VMEM((2, 8, mig), f32),
            pltpu.VMEM((2, 8, mig), f32),
            pltpu.SemaphoreType.DMA((2,)),
            pltpu.SemaphoreType.DMA((2,)),
            pltpu.SemaphoreType.DMA((slots,)),
            pltpu.SemaphoreType.DMA((slots,)),
        ],
        compiler_params=pltpu.CompilerParams(collective_id=0, has_side_effects=True),
    )(sigma_table, depth_table, charge_table, domain_edge, fraction, atom_type, perturbed, leaving)
    forces, sums = pl.pallas_call(
        bound(pair_kernel, sizes),
        name="pairs",
        out_shape=(
            jax.ShapeDtypeStruct(fraction.shape, f32),
            jax.ShapeDtypeStruct((3, 8, LANES), f32),
        ),
        in_specs=[smem] * 4 + [vmem],
        out_specs=(vmem, vmem),
        scratch_shapes=[
            pltpu.VMEM((9, LANES, LANES), f32),
            pltpu.VMEM((3, LANES, LANES), f32),
        ],
    )(neighbours, counts, domain_edge, coupling, ghosts)
    total = nx * ny * nz
    energy, dhdl = pl.pallas_call(
        bound(sum_kernel, sizes, atoms),
        name="window_sum",
        out_shape=(jax.ShapeDtypeStruct((1,), f32), jax.ShapeDtypeStruct((1,), f32)),
        in_specs=[smem, vmem],
        out_specs=(smem, smem),
        scratch_shapes=[
            pltpu.VMEM((8, LANES), f32),
            pltpu.VMEM((total, 8, LANES), f32),
            pltpu.SemaphoreType.DMA((total,)),
            pltpu.SemaphoreType.DMA((total,)),
        ],
        compiler_params=pltpu.CompilerParams(collective_id=1, has_side_effects=True),
    )(coupling, sums)
    return forces, energy, dhdl


def solution(mesh):
    sizes = (mesh.shape["dx"], mesh.shape["dy"], mesh.shape["dz"])
    return jax.shard_map(
        lambda *arrays: on_device(sizes, *arrays),
        mesh=mesh,
        in_specs=(
            P(None, ("win", "dx"), "dy", "dz", None),
            P(("win", "dx"), "dy", "dz", None),
            P(("win", "dx"), "dy", "dz", None),
            P(("win", "dx"), "dy", "dz", None, None),
            P(("win", "dx"), "dy", "dz", None, None),
            P(("win", "dx"), "dy", "dz", None),
            P(),
            P(),
            P(),
            P(),
            P("win"),
        ),
        out_specs=(P(None, ("win", "dx"), "dy", "dz", None), P("win"), P("win")),
        check_vma=False,
    )
```

```python
import jax
import jax.numpy as jnp
from jax import lax
from jax.experimental import pallas as pl
from jax.experimental.pallas import tpu as pltpu
from jax.sharding import PartitionSpec as P

soft_base = 0.3
soft_alpha = 0.5
charge_base = 0.3
charge_alpha = 0.5
coulomb = 0.1
LANES = 128
MESH = pl.DeviceIdType.MESH
HIGHEST = lax.Precision.HIGHEST


def steps_of(count):
    return {1: (0,), 2: (0, 1)}.get(count, (-1, 0, 1))


def slot_step(step, count):
    if count == 1:
        return step * 0
    if count == 2:
        return step * step
    return step + 1


def thirds(value):
    high = value.astype(jnp.bfloat16).astype(jnp.float32)
    rest = value - high
    middle = rest.astype(jnp.bfloat16).astype(jnp.float32)
    return jnp.concatenate([high, middle, rest - middle], axis=0)


def joined(value):
    return value[0:8] + value[8:16] + value[16:24]


def halo_kernel(
    sizes,
    edge_ref,
    fraction_ref,
    type_ref,
    flag_ref,
    leaving_ref,
    ghost_ref,
    outgoing,
    incoming,
    mig_send,
    mig_recv,
    send_sem,
    recv_sem,
):
    nx, ny, nz = sizes
    atoms = fraction_ref.shape[-1]
    spacing = float(atoms) ** (1.0 / 3.0)
    me = (lax.axis_index("dx"), lax.axis_index("dy"), lax.axis_index("dz"))

    def device(step):
        return {
            name: lax.rem(place + by + count, count)
            for name, place, by, count in zip(("dx", "dy", "dz"), me, step, sizes)
        }

    offsets = [(a, b, c) for a in steps_of(nx) for b in steps_of(ny) for c in steps_of(nz)]
    others = [o for o in offsets if any(o)]

    def slot(o):
        return (
            slot_step(o[0], nx) * len(steps_of(ny)) + slot_step(o[1], ny)
        ) * len(steps_of(nz)) + slot_step(o[2], nz)

    barrier = pltpu.get_barrier_semaphore()
    for o in others:
        pl.semaphore_signal(
            barrier, inc=1, device_id=device(tuple(-x for x in o)), device_id_type=MESH
        )

    own = ghost_ref.at[slot((0, 0, 0))]
    edge = [edge_ref[k] * spacing for k in range(3)]
    rows = [fraction_ref[k, 0, 0] * edge[k] for k in range(3)]
    rows += [type_ref[0, 0].astype(jnp.float32), flag_ref[0, 0].astype(jnp.float32)]
    payload = jnp.concatenate(rows + [jnp.zeros((3, atoms), jnp.float32)], axis=0)
    leave = leaving_ref[0, 0, 0]
    mig = leave.shape[1]
    slots_in = jnp.concatenate([leave[0:1], leave[1:2]], axis=1)
    slots_out = jnp.concatenate([leave[1:2], leave[0:1]], axis=1)
    place = lax.broadcasted_iota(jnp.int32, (atoms, 2 * mig), 0)
    hot_in = (place == slots_in).astype(jnp.float32).astype(jnp.bfloat16)
    hot_out = (place == slots_out).astype(jnp.float32).astype(jnp.bfloat16)
    lane = lax.broadcasted_iota(jnp.int32, (8, 2 * mig), 1)
    first = lax.broadcasted_iota(jnp.int32, (8, 2 * mig), 0) == 0
    shift = jnp.where(first, jnp.where(lane < mig, edge[0], -edge[0]), 0.0)
    leavers = joined(
        jnp.dot(thirds(payload).astype(jnp.bfloat16), hot_out, preferred_element_type=jnp.float32)
    )
    outgoing[...] = leavers + shift

    def spread(value):
        return lax.dot_general(
            value.astype(jnp.bfloat16),
            hot_in,
            (((1,), (1,)), ((), ())),
            preferred_element_type=jnp.float32,
        )

    gone = spread(jnp.ones((8, 2 * mig), jnp.float32))

    pl.semaphore_wait(barrier, len(others))
    moves = []
    for side, by in ((0, 1), (1, -1)):
        move = pltpu.make_async_remote_copy(
            src_ref=outgoing,
            dst_ref=incoming.at[side],
            send_sem=mig_send.at[side],
            recv_sem=mig_recv.at[side],
            device_id=device((by, 0, 0)),
            device_id_type=MESH,
        )
        move.start()
        moves.append(move)
    for move in moves:
        move.wait()
    merged = jnp.where(lane < mig, incoming[1], incoming[0])
    moved = jnp.where(gone > 0.5, joined(spread(thirds(merged))), payload)
    for r in range(5):
        own[r] = moved[r : r + 1]
    copies = []
    for k, o in enumerate(sorted(others, key=lambda o: -sum(map(abs, o)))):
        copy = pltpu.make_async_remote_copy(
            src_ref=own,
            dst_ref=ghost_ref.at[slot(o)],
            send_sem=send_sem.at[k],
            recv_sem=recv_sem.at[k],
            device_id=device(tuple(-x for x in o)),
            device_id_type=MESH,
        )
        copy.start()
        copies.append(copy)
    for copy in copies:
        copy.wait()


def pair_kernel(
    sizes,
    listed_ref,
    count_ref,
    edge_ref,
    coupling_ref,
    sigma_ref,
    depth_ref,
    charge_ref,
    ghost_ref,
    force_ref,
    sums_ref,
    own_cols,
    force_acc,
    params,
):
    nx, ny, nz = sizes
    atoms = ghost_ref.shape[-1]
    blocks = atoms // LANES
    spacing = float(atoms) ** (1.0 / 3.0)
    edge = [edge_ref[k] * spacing for k in range(3)]
    lam = coupling_ref[0]
    own_slot = (slot_step(0, nx) * len(steps_of(ny)) + slot_step(0, ny)) * len(
        steps_of(nz)
    ) + slot_step(0, nz)
    ones = jnp.ones((8, LANES), jnp.bfloat16)
    for k in range(3):
        sums_ref[k] = jnp.zeros((8, LANES), jnp.float32)

    lane = lax.broadcasted_iota(jnp.int32, (1, LANES), 1)
    tables = [jnp.zeros((1, LANES), jnp.float32)] * 3
    for k in range(sigma_ref.shape[0]):
        hit = lane == k
        tables = [
            jnp.where(hit, ref[k], table)
            for ref, table in zip((sigma_ref, depth_ref, charge_ref), tables)
        ]
    table = jnp.concatenate(
        [tables[0] * 0.5, jnp.sqrt(tables[1]) * 2.0, tables[2]] + [tables[2] * 0.0] * 5, axis=0
    )
    for place in range(ghost_ref.shape[0]):
        for q in range(blocks):
            span = slice(q * LANES, (q + 1) * LANES)
            kind = ghost_ref[place, 3, :, span].astype(jnp.int32)
            params[place, :, span] = jnp.take_along_axis(
                table, jnp.broadcast_to(kind, (8, LANES)), axis=1, mode="promise_in_bounds"
            )
    picks = (
        lax.broadcasted_iota(jnp.int32, (24, 7 * LANES), 0) % 8
        == lax.broadcasted_iota(jnp.int32, (24, 7 * LANES), 1) // LANES
    ).astype(jnp.float32).astype(jnp.bfloat16)
    for q in range(blocks):
        span = slice(q * LANES, (q + 1) * LANES)
        known = params[own_slot, :, span]
        rows = [ghost_ref[own_slot, r, :, span] for r in range(3)]
        rows += [known[0:1], known[1:2], known[2:3] * coulomb]
        rows += [ghost_ref[own_slot, 4, :, span], known[3:4]]
        cols = thirds(jnp.concatenate(rows, axis=0)).T.astype(jnp.bfloat16)
        wide = jnp.dot(cols, picks, preferred_element_type=jnp.float32)
        for r in range(7):
            own_cols[q, r] = wide[:, r * LANES : (r + 1) * LANES]
    for q in range(blocks):
        for k in range(3):
            force_acc[q, k] = jnp.zeros((LANES, LANES), jnp.float32)

    @pl.loop(0, blocks)
    def _(q):
        @pl.loop(0, count_ref[0, 0, 0, q])
        def _(e):
            listed = listed_ref[q, 0, e]
            image = lax.div(listed, blocks)
            start = pl.multiple_of(lax.rem(listed, blocks) * LANES, LANES)
            a = lax.div(image, 9) - 1
            b = lax.rem(lax.div(image, 3), 3) - 1
            c = lax.rem(image, 3) - 1
            where_from = (
                slot_step(a, nx) * len(steps_of(ny)) + slot_step(b, ny)
            ) * len(steps_of(nz)) + slot_step(c, nz)
            rows = []
            for r in range(7):
                if 3 <= r < 6:
                    row = params[where_from, pl.ds(r - 3, 1), pl.ds(start, LANES)]
                else:
                    row = ghost_ref[where_from, min(r, 4), :, pl.ds(start, LANES)]
                if r < 3:
                    row = row + (a, b, c)[r].astype(jnp.float32) * edge[r]
                rows.append(jnp.broadcast_to(row, (8, LANES)))
            xj, yj, zj, hj, ej, qj, pj = rows

            def terms(masked):
                tot = jnp.zeros((8, LANES), jnp.float32)
                tot_p = jnp.zeros((8, LANES), jnp.float32)
                tot_k = jnp.zeros((8, LANES), jnp.float32)
                for g in range(LANES // 8):
                    at = pl.ds(g * 8, 8)
                    dx = own_cols[q, 0, at] - xj
                    dy = own_cols[q, 1, at] - yj
                    dz = own_cols[q, 2, at] - zj
                    r2 = dx * dx + dy * dy + dz * dz
                    sig = own_cols[q, 3, at] + hj
                    s2 = sig * sig
                    s6 = s2 * s2 * s2
                    eps4 = own_cols[q, 4, at] * ej
                    qq = own_cols[q, 5, at] * qj
                    if masked:
                        diag = (
                            lax.broadcasted_iota(jnp.int32, (8, LANES), 0) + g * 8
                            == lax.broadcasted_iota(jnp.int32, (8, LANES), 1)
                        )
                        eps4 = jnp.where(diag, 0.0, eps4)
                        qq = jnp.where(diag, 0.0, qq)
                    p = jnp.maximum(own_cols[q, 6, at], pj)
                    soft = soft_base + (soft_alpha * lam) * p
                    weight = 1.0 - lam * p
                    r4 = r2 * r2
                    soft6 = s6 * soft + r4 * r2
                    inv = 1.0 / soft6
                    u = lax.rsqrt(soft + r2)
                    ec = qq * u
                    half = (0.5 * ec) * (u * u)
                    t = s6 * inv
                    et = eps4 * t
                    tm = t - 1.0
                    v = et * tm + ec
                    m = et * (t + tm)
                    kk = m * t + half
                    fs = weight * (3.0 * (m * (r4 * inv)) + half)
                    tot = tot + v
                    tot_p = tot_p + p * v
                    tot_k = tot_k + p * kk
                    force_acc[q, 0, at] += fs * dx
                    force_acc[q, 1, at] += fs * dy
                    force_acc[q, 2, at] += fs * dz
                sums_ref[0] += tot
                sums_ref[1] += tot_p
                sums_ref[2] += tot_k

            is_self = listed == 13 * blocks + q

            @pl.when(is_self)
            def _():
                terms(True)

            @pl.when(jnp.logical_not(is_self))
            def _():
                terms(False)

    for q in range(blocks):
        for k in range(3):
            whole = force_acc[q, k]
            high = whole.astype(jnp.bfloat16)
            low = (whole - high.astype(jnp.float32)).astype(jnp.bfloat16)
            total = sum(
                lax.dot_general(
                    ones, part, (((1,), (1,)), ((), ())), preferred_element_type=jnp.float32
                )
                for part in (high, low)
            )
            force_ref[k, 0, 0, :, q * LANES : (q + 1) * LANES] = 2.0 * total[0:1]


def sum_kernel(sizes, atoms, coupling_ref, sums_ref, energy_ref, dhdl_ref, tile, gathered, send_sem, recv_sem):
    nx, ny, nz = sizes
    total = nx * ny * nz
    me = (lax.axis_index("dx") * ny + lax.axis_index("dy")) * nz + lax.axis_index("dz")

    def device(k):
        return {"dx": k // (ny * nz), "dy": k // nz % ny, "dz": k % nz}

    barrier = pltpu.get_barrier_semaphore()

    @pl.loop(1, total)
    def _(by):
        pl.semaphore_signal(
            barrier, inc=1, device_id=device(lax.rem(me + by, total)), device_id_type=MESH
        )

    rows = [jnp.sum(sums_ref[k], axis=0, keepdims=True) for k in range(3)]
    rows.append(jnp.zeros((5, LANES), jnp.float32))
    tile[...] = jnp.concatenate(rows, axis=0)
    gathered[me] = tile[...]
    pl.semaphore_wait(barrier, total - 1)

    def copy(by):
        return pltpu.make_async_remote_copy(
            src_ref=tile,
            dst_ref=gathered.at[me],
            send_sem=send_sem.at[by],
            recv_sem=recv_sem.at[by],
            device_id=device(lax.rem(me + by, total)),
            device_id_type=MESH,
        )

    @pl.loop(1, total)
    def _(by):
        copy(by).start()

    @pl.loop(1, total)
    def _(by):
        copy(by).wait()

    summed = jnp.sum(gathered[...], axis=0)
    whole = [jnp.sum(summed[k : k + 1]) for k in range(3)]
    lam = coupling_ref[0]
    scale = 0.5 / float(atoms * total)
    energy_ref[0] = scale * (whole[0] - lam * whole[1])
    dhdl_ref[0] = -scale * (whole[1] + (0.5 * (1.0 - lam)) * whole[2])


def on_device(sizes, fraction, atom_type, perturbed, leaving, neighbours, counts,
              sigma_table, depth_table, charge_table, domain_edge, coupling):
    nx, ny, nz = sizes
    atoms = fraction.shape[-1]
    mig = leaving.shape[-1]
    slots = len(steps_of(nx)) * len(steps_of(ny)) * len(steps_of(nz))
    smem = pl.BlockSpec(memory_space=pltpu.SMEM)
    vmem = pl.BlockSpec(memory_space=pltpu.VMEM)
    f32 = jnp.float32

    def bound(kernel, *values):
        return lambda *refs: kernel(*values, *refs)

    ghosts = pl.pallas_call(
        bound(halo_kernel, sizes),
        name="halo",
        out_shape=jax.ShapeDtypeStruct((slots, 5, 1, atoms), f32),
        in_specs=[smem] + [vmem] * 4,
        out_specs=vmem,
        scratch_shapes=[
            pltpu.VMEM((8, 2 * mig), f32),
            pltpu.VMEM((2, 8, 2 * mig), f32),
            pltpu.SemaphoreType.DMA((2,)),
            pltpu.SemaphoreType.DMA((2,)),
            pltpu.SemaphoreType.DMA((slots,)),
            pltpu.SemaphoreType.DMA((slots,)),
        ],
        compiler_params=pltpu.CompilerParams(collective_id=0, has_side_effects=True),
    )(domain_edge, fraction, atom_type, perturbed, leaving)
    forces, sums = pl.pallas_call(
        bound(pair_kernel, sizes),
        name="pairs",
        out_shape=(
            jax.ShapeDtypeStruct(fraction.shape, f32),
            jax.ShapeDtypeStruct((3, 8, LANES), f32),
        ),
        in_specs=[smem] * 7 + [vmem],
        out_specs=(vmem, vmem),
        scratch_shapes=[
            pltpu.VMEM((atoms // LANES, 7, LANES, LANES), f32),
            pltpu.VMEM((atoms // LANES, 3, LANES, LANES), f32),
            pltpu.VMEM((slots, 8, atoms), f32),
        ],
    )(neighbours.reshape(atoms // LANES, 1, -1), counts, domain_edge, coupling, sigma_table, depth_table, charge_table, ghosts)
    total = nx * ny * nz
    energy, dhdl = pl.pallas_call(
        bound(sum_kernel, sizes, atoms),
        name="window_sum",
        out_shape=(jax.ShapeDtypeStruct((1,), f32), jax.ShapeDtypeStruct((1,), f32)),
        in_specs=[smem, vmem],
        out_specs=(smem, smem),
        scratch_shapes=[
            pltpu.VMEM((8, LANES), f32),
            pltpu.VMEM((total, 8, LANES), f32),
            pltpu.SemaphoreType.DMA((total,)),
            pltpu.SemaphoreType.DMA((total,)),
        ],
        compiler_params=pltpu.CompilerParams(collective_id=1, has_side_effects=True),
    )(coupling, sums)
    return forces, energy, dhdl


def solution(mesh):
    sizes = (mesh.shape["dx"], mesh.shape["dy"], mesh.shape["dz"])
    return jax.shard_map(
        lambda *arrays: on_device(sizes, *arrays),
        mesh=mesh,
        in_specs=(
            P(None, ("win", "dx"), "dy", "dz", None),
            P(("win", "dx"), "dy", "dz", None),
            P(("win", "dx"), "dy", "dz", None),
            P(("win", "dx"), "dy", "dz", None, None),
            P(("win", "dx"), "dy", "dz", None, None),
            P(("win", "dx"), "dy", "dz", None),
            P(),
            P(),
            P(),
            P(),
            P("win"),
        ),
        out_specs=(P(None, ("win", "dx"), "dy", "dz", None), P("win"), P("win")),
        check_vma=False,
    )
```

```python
import jax
import jax.numpy as jnp
from jax import lax
from jax.experimental import pallas as pl
from jax.experimental.pallas import tpu as pltpu
from jax.sharding import PartitionSpec as P

soft_base = 0.3
soft_alpha = 0.5
charge_base = 0.3
charge_alpha = 0.5
coulomb = 0.1
LANES = 128
MESH = pl.DeviceIdType.MESH
HIGHEST = lax.Precision.HIGHEST


def steps_of(count):
    return {1: (0,), 2: (0, 1)}.get(count, (-1, 0, 1))


def slot_step(step, count):
    if count == 1:
        return step * 0
    if count == 2:
        return step * step
    return step + 1


def thirds(value):
    high = value.astype(jnp.bfloat16).astype(jnp.float32)
    rest = value - high
    middle = rest.astype(jnp.bfloat16).astype(jnp.float32)
    return jnp.concatenate([high, middle, rest - middle], axis=0)


def joined(value):
    return value[0:8] + value[8:16] + value[16:24]


def step_kernel(
    sizes,
    edge_ref,
    coupling_ref,
    sigma_ref,
    depth_ref,
    charge_ref,
    listed_ref,
    count_ref,
    fraction_ref,
    type_ref,
    flag_ref,
    leaving_ref,
    force_ref,
    energy_ref,
    dhdl_ref,
    ghost_ref,
    outgoing,
    incoming,
    own_cols,
    force_acc,
    params,
    sums_ref,
    tile,
    gathered,
    mig_send,
    mig_recv,
    send_sem,
    recv_sem,
    sum_send,
    sum_recv,
):
    nx, ny, nz = sizes
    atoms = fraction_ref.shape[-1]
    spacing = float(atoms) ** (1.0 / 3.0)
    me = (lax.axis_index("dx"), lax.axis_index("dy"), lax.axis_index("dz"))

    def device(step):
        return {
            name: lax.rem(place + by + count, count)
            for name, place, by, count in zip(("dx", "dy", "dz"), me, step, sizes)
        }

    offsets = [(a, b, c) for a in steps_of(nx) for b in steps_of(ny) for c in steps_of(nz)]
    others = [o for o in offsets if any(o)]

    def slot(o):
        return (
            slot_step(o[0], nx) * len(steps_of(ny)) + slot_step(o[1], ny)
        ) * len(steps_of(nz)) + slot_step(o[2], nz)

    barrier = pltpu.get_barrier_semaphore()
    total = nx * ny * nz
    my_id = (me[0] * ny + me[1]) * nz + me[2]

    def window_device(k):
        return {
            "dx": lax.div(k, ny * nz),
            "dy": lax.rem(lax.div(k, nz), ny),
            "dz": lax.rem(k, nz),
        }

    @pl.loop(1, total)
    def _(by):
        pl.semaphore_signal(
            barrier,
            inc=1,
            device_id=window_device(lax.rem(my_id + by, total)),
            device_id_type=MESH,
        )

    own = ghost_ref.at[slot((0, 0, 0))]
    edge = [edge_ref[k] * spacing for k in range(3)]
    rows = [fraction_ref[k, 0, 0] * edge[k] for k in range(3)]
    rows += [type_ref[0, 0].astype(jnp.float32), flag_ref[0, 0].astype(jnp.float32)]
    payload = jnp.concatenate(rows + [jnp.zeros((3, atoms), jnp.float32)], axis=0)
    leave = leaving_ref[0, 0, 0]
    mig = leave.shape[1]
    slots_in = jnp.concatenate([leave[0:1], leave[1:2]], axis=1)
    slots_out = jnp.concatenate([leave[1:2], leave[0:1]], axis=1)
    place = lax.broadcasted_iota(jnp.int32, (atoms, 2 * mig), 0)
    hot_in = (place == slots_in).astype(jnp.float32).astype(jnp.bfloat16)
    hot_out = (place == slots_out).astype(jnp.float32).astype(jnp.bfloat16)
    lane = lax.broadcasted_iota(jnp.int32, (8, 2 * mig), 1)
    first = lax.broadcasted_iota(jnp.int32, (8, 2 * mig), 0) == 0
    shift = jnp.where(first, jnp.where(lane < mig, edge[0], -edge[0]), 0.0)
    leavers = joined(
        jnp.dot(thirds(payload).astype(jnp.bfloat16), hot_out, preferred_element_type=jnp.float32)
    )
    outgoing[...] = leavers + shift

    def spread(value):
        return lax.dot_general(
            value.astype(jnp.bfloat16),
            hot_in,
            (((1,), (1,)), ((), ())),
            preferred_element_type=jnp.float32,
        )

    gone = spread(jnp.ones((8, 2 * mig), jnp.float32))

    pl.semaphore_wait(barrier, total - 1)
    moves = []
    for side, by in ((0, 1), (1, -1)):
        move = pltpu.make_async_remote_copy(
            src_ref=outgoing,
            dst_ref=incoming.at[side],
            send_sem=mig_send.at[side],
            recv_sem=mig_recv.at[side],
            device_id=device((by, 0, 0)),
            device_id_type=MESH,
        )
        move.start()
        moves.append(move)
    for move in moves:
        move.wait()
    merged = jnp.where(lane < mig, incoming[1], incoming[0])
    moved = jnp.where(gone > 0.5, joined(spread(thirds(merged))), payload)
    for r in range(5):
        own[r] = moved[r : r + 1]
    copies = []
    for k, o in enumerate(sorted(others, key=lambda o: -sum(map(abs, o)))):
        copy = pltpu.make_async_remote_copy(
            src_ref=own,
            dst_ref=ghost_ref.at[slot(o)],
            send_sem=send_sem.at[k],
            recv_sem=recv_sem.at[k],
            device_id=device(tuple(-x for x in o)),
            device_id_type=MESH,
        )
        copy.start()
        copies.append((copy, slot(o)))

    blocks = atoms // LANES
    lam = coupling_ref[0]
    own_slot = slot((0, 0, 0))
    ones = jnp.ones((8, LANES), jnp.bfloat16)
    for k in range(3):
        sums_ref[k] = jnp.zeros((8, LANES), jnp.float32)

    ahead = lax.broadcasted_iota(jnp.int32, (8, LANES), 1) - lax.broadcasted_iota(
        jnp.int32, (8, LANES), 0
    )
    lane = lax.broadcasted_iota(jnp.int32, (1, LANES), 1)
    tables = [jnp.zeros((1, LANES), jnp.float32)] * 3
    for k in range(sigma_ref.shape[0]):
        hit = lane == k
        tables = [
            jnp.where(hit, ref[k], table)
            for ref, table in zip((sigma_ref, depth_ref, charge_ref), tables)
        ]
    table = jnp.concatenate(
        [tables[0] * 0.5, jnp.sqrt(tables[1]) * 2.0, tables[2]] + [tables[2] * 0.0] * 5, axis=0
    )
    kinds = sigma_ref.shape[0]
    table_parts = thirds(table[:, :kinds]).astype(jnp.bfloat16)
    kind_row = lax.broadcasted_iota(jnp.int32, (kinds, atoms), 0).astype(jnp.float32)

    def look_up(place):
        onehot = (kind_row == ghost_ref[place, 3]).astype(jnp.float32).astype(jnp.bfloat16)
        found = joined(jnp.dot(table_parts, onehot, preferred_element_type=jnp.float32))
        rows = [ghost_ref[place, r] for r in range(3)]
        rows += [found[0:3], ghost_ref[place, 4], found[3:4]]
        whole = jnp.concatenate(rows, axis=0)
        for q in range(blocks):
            params[place * blocks + q] = whole[:, q * LANES : (q + 1) * LANES]

    look_up(own_slot)
    picks = (
        lax.broadcasted_iota(jnp.int32, (24, 7 * LANES), 0) % 8
        == lax.broadcasted_iota(jnp.int32, (24, 7 * LANES), 1) // LANES
    ).astype(jnp.float32).astype(jnp.bfloat16)
    for q in range(blocks):
        cols = thirds(params[own_slot * blocks + q]).T.astype(jnp.bfloat16)
        wide = jnp.dot(cols, picks, preferred_element_type=jnp.float32)
        for r in range(7):
            col = wide[:, r * LANES : (r + 1) * LANES]
            own_cols[q, r] = col * coulomb if r == 5 else col
    for q in range(blocks):
        for k in range(3):
            force_acc[q, k] = jnp.zeros((LANES, LANES), jnp.float32)

    for copy, place in copies:
        copy.wait()
        look_up(place)

    @pl.loop(0, blocks)
    def _(q):
        def entry(e):
            listed = listed_ref[q, 0, e]
            left = jnp.minimum(jnp.maximum(count_ref[0, 0, 0, q] - e, 0), 1)
            used = left.astype(jnp.float32)
            apart = jnp.abs(listed - (13 * blocks + q))
            self_lane = jnp.minimum(apart, 1) * (2 * LANES)
            image = lax.div(listed, blocks)
            a = lax.div(image, 9) - 1
            b = lax.rem(lax.div(image, 3), 3) - 1
            c = lax.rem(image, 3) - 1
            where_from = (
                slot_step(a, nx) * len(steps_of(ny)) + slot_step(b, ny)
            ) * len(steps_of(nz)) + slot_step(c, nz)
            other = params[where_from * blocks + lax.rem(listed, blocks)]
            rows = []
            for r in range(7):
                row = other[r : r + 1]
                if r < 3:
                    row = row + (a, b, c)[r].astype(jnp.float32) * edge[r]
                if 4 <= r < 6:
                    row = row * used
                rows.append(jnp.broadcast_to(row, (8, LANES)))
            xj, yj, zj, hj, ej, qj, pj = rows

            tot = jnp.zeros((8, LANES), jnp.float32)
            tot_p = jnp.zeros((8, LANES), jnp.float32)
            tot_k = jnp.zeros((8, LANES), jnp.float32)
            for g in range(LANES // 8):
                at = pl.ds(g * 8, 8)
                dx = own_cols[q, 0, at] - xj
                dy = own_cols[q, 1, at] - yj
                dz = own_cols[q, 2, at] - zj
                r2 = dx * dx + dy * dy + dz * dz
                sig = own_cols[q, 3, at] + hj
                s2 = sig * sig
                s6 = s2 * s2 * s2
                eps4 = own_cols[q, 4, at] * ej
                qq = own_cols[q, 5, at] * qj
                diag = ahead == self_lane + g * 8
                eps4 = jnp.where(diag, 0.0, eps4)
                qq = jnp.where(diag, 0.0, qq)
                p = jnp.maximum(own_cols[q, 6, at], pj)
                soft = soft_base + (soft_alpha * lam) * p
                weight = 1.0 - lam * p
                r4 = r2 * r2
                soft6 = s6 * soft + r4 * r2
                inv = 1.0 / soft6
                u = lax.rsqrt(soft + r2)
                ec = qq * u
                half = (0.5 * ec) * (u * u)
                t = s6 * inv
                et = eps4 * t
                tm = t - 1.0
                v = et * tm + ec
                m = et * (t + tm)
                kk = m * t + half
                fs = weight * (3.0 * (m * (r4 * inv)) + half)
                tot = tot + v
                tot_p = tot_p + p * v
                tot_k = tot_k + p * kk
                force_acc[q, 0, at] += fs * dx
                force_acc[q, 1, at] += fs * dy
                force_acc[q, 2, at] += fs * dz
            sums_ref[0] += tot
            sums_ref[1] += tot_p
            sums_ref[2] += tot_k

        width = listed_ref.shape[-1]
        unroll = 2 if width % 2 == 0 else 1

        @pl.loop(0, width // unroll)
        def _(step):
            for k in range(unroll):
                entry(step * unroll + k)

    folded = [jnp.sum(sums_ref[k], axis=0, keepdims=True) for k in range(3)]
    folded.append(jnp.zeros((5, LANES), jnp.float32))
    mine = jnp.concatenate(folded, axis=0)
    tile[...] = mine
    gathered[my_id] = mine

    def share(by):
        return pltpu.make_async_remote_copy(
            src_ref=tile,
            dst_ref=gathered.at[my_id],
            send_sem=sum_send.at[by],
            recv_sem=sum_recv.at[by],
            device_id=window_device(lax.rem(my_id + by, total)),
            device_id_type=MESH,
        )

    @pl.loop(1, total)
    def _(by):
        share(by).start()

    for q in range(blocks):
        for k in range(3):
            whole = force_acc[q, k]
            high = whole.astype(jnp.bfloat16)
            low = (whole - high.astype(jnp.float32)).astype(jnp.bfloat16)
            reduced = sum(
                lax.dot_general(
                    ones, part, (((1,), (1,)), ((), ())), preferred_element_type=jnp.float32
                )
                for part in (high, low)
            )
            force_ref[k, 0, 0, :, q * LANES : (q + 1) * LANES] = 2.0 * reduced[0:1]

    @pl.loop(1, total)
    def _(by):
        share(by).wait()

    summed = jnp.sum(gathered[...], axis=0)
    parts = [jnp.sum(summed[k : k + 1]) for k in range(3)]
    scale = 0.5 / float(atoms * total)
    energy_ref[0] = scale * (parts[0] - lam * parts[1])
    dhdl_ref[0] = -scale * (parts[1] + (0.5 * (1.0 - lam)) * parts[2])


def on_device(sizes, fraction, atom_type, perturbed, leaving, neighbours, counts,
              sigma_table, depth_table, charge_table, domain_edge, coupling):
    nx, ny, nz = sizes
    atoms = fraction.shape[-1]
    mig = leaving.shape[-1]
    slots = len(steps_of(nx)) * len(steps_of(ny)) * len(steps_of(nz))
    smem = pl.BlockSpec(memory_space=pltpu.SMEM)
    vmem = pl.BlockSpec(memory_space=pltpu.VMEM)
    f32 = jnp.float32

    def bound(kernel, *values):
        return lambda *refs: kernel(*values, *refs)

    blocks = atoms // LANES
    total = nx * ny * nz
    dma = pltpu.SemaphoreType.DMA
    return pl.pallas_call(
        bound(step_kernel, sizes),
        name="step",
        out_shape=(
            jax.ShapeDtypeStruct(fraction.shape, f32),
            jax.ShapeDtypeStruct((1,), f32),
            jax.ShapeDtypeStruct((1,), f32),
        ),
        in_specs=[smem] * 7 + [vmem] * 4,
        out_specs=(vmem, smem, smem),
        scratch_shapes=[
            pltpu.VMEM((slots, 5, 1, atoms), f32),
            pltpu.VMEM((8, 2 * mig), f32),
            pltpu.VMEM((2, 8, 2 * mig), f32),
            pltpu.VMEM((blocks, 7, LANES, LANES), f32),
            pltpu.VMEM((blocks, 3, LANES, LANES), f32),
            pltpu.VMEM((slots * blocks, 8, LANES), f32),
            pltpu.VMEM((3, 8, LANES), f32),
            pltpu.VMEM((8, LANES), f32),
            pltpu.VMEM((total, 8, LANES), f32),
            dma((2,)),
            dma((2,)),
            dma((slots,)),
            dma((slots,)),
            dma((total,)),
            dma((total,)),
        ],
        compiler_params=pltpu.CompilerParams(collective_id=0, has_side_effects=True),
    )(
        domain_edge,
        coupling,
        sigma_table,
        depth_table,
        charge_table,
        neighbours.reshape(blocks, 1, -1),
        counts,
        fraction,
        atom_type,
        perturbed,
        leaving,
    )


def solution(mesh):
    sizes = (mesh.shape["dx"], mesh.shape["dy"], mesh.shape["dz"])
    return jax.shard_map(
        lambda *arrays: on_device(sizes, *arrays),
        mesh=mesh,
        in_specs=(
            P(None, ("win", "dx"), "dy", "dz", None),
            P(("win", "dx"), "dy", "dz", None),
            P(("win", "dx"), "dy", "dz", None),
            P(("win", "dx"), "dy", "dz", None, None),
            P(("win", "dx"), "dy", "dz", None, None),
            P(("win", "dx"), "dy", "dz", None),
            P(),
            P(),
            P(),
            P(),
            P("win"),
        ),
        out_specs=(P(None, ("win", "dx"), "dy", "dz", None), P("win"), P("win")),
        check_vma=False,
    )
```

```python
import jax
import jax.numpy as jnp
from jax import lax
from jax.experimental import pallas as pl
from jax.experimental.pallas import tpu as pltpu
from jax.sharding import PartitionSpec as P

soft_base = 0.3
soft_alpha = 0.5
charge_base = 0.3
charge_alpha = 0.5
coulomb = 0.1
LANES = 128
MESH = pl.DeviceIdType.MESH
HIGHEST = lax.Precision.HIGHEST


def steps_of(count):
    return {1: (0,), 2: (0, 1)}.get(count, (-1, 0, 1))


def slot_step(step, count):
    if count == 1:
        return step * 0
    if count == 2:
        return step * step
    return step + 1


def thirds(value):
    high = value.astype(jnp.bfloat16).astype(jnp.float32)
    rest = value - high
    middle = rest.astype(jnp.bfloat16).astype(jnp.float32)
    return jnp.concatenate([high, middle, rest - middle], axis=0)


def joined(value):
    return value[0:8] + value[8:16] + value[16:24]


def step_kernel(
    sizes,
    edge_ref,
    coupling_ref,
    sigma_ref,
    depth_ref,
    charge_ref,
    listed_ref,
    count_ref,
    fraction_ref,
    type_ref,
    flag_ref,
    leaving_ref,
    force_ref,
    energy_ref,
    dhdl_ref,
    ghost_ref,
    outgoing,
    incoming,
    own_cols,
    force_acc,
    params,
    sums_ref,
    tile,
    gathered,
    mig_send,
    mig_recv,
    send_sem,
    recv_sem,
    sum_send,
    sum_recv,
):
    nx, ny, nz = sizes
    atoms = fraction_ref.shape[-1]
    spacing = float(atoms) ** (1.0 / 3.0)
    me = (lax.axis_index("dx"), lax.axis_index("dy"), lax.axis_index("dz"))

    def device(step):
        return {
            name: lax.rem(place + by + count, count)
            for name, place, by, count in zip(("dx", "dy", "dz"), me, step, sizes)
        }

    offsets = [(a, b, c) for a in steps_of(nx) for b in steps_of(ny) for c in steps_of(nz)]
    others = [o for o in offsets if any(o)]

    def slot(o):
        return (
            slot_step(o[0], nx) * len(steps_of(ny)) + slot_step(o[1], ny)
        ) * len(steps_of(nz)) + slot_step(o[2], nz)

    barrier = pltpu.get_barrier_semaphore()
    total = nx * ny * nz
    my_id = (me[0] * ny + me[1]) * nz + me[2]

    def window_device(k):
        return {
            "dx": lax.div(k, ny * nz),
            "dy": lax.rem(lax.div(k, nz), ny),
            "dz": lax.rem(k, nz),
        }

    @pl.loop(1, total)
    def _(by):
        pl.semaphore_signal(
            barrier,
            inc=1,
            device_id=window_device(lax.rem(my_id + by, total)),
            device_id_type=MESH,
        )

    own = ghost_ref.at[slot((0, 0, 0))]
    edge = [edge_ref[k] * spacing for k in range(3)]
    rows = [fraction_ref[k, 0, 0] * edge[k] for k in range(3)]
    rows += [type_ref[0, 0].astype(jnp.float32), flag_ref[0, 0].astype(jnp.float32)]
    payload = jnp.concatenate(rows + [jnp.zeros((3, atoms), jnp.float32)], axis=0)
    leave = leaving_ref[0, 0, 0]
    mig = leave.shape[1]
    slots_in = jnp.concatenate([leave[0:1], leave[1:2]], axis=1)
    slots_out = jnp.concatenate([leave[1:2], leave[0:1]], axis=1)
    place = lax.broadcasted_iota(jnp.int32, (atoms, 2 * mig), 0)
    hot_in = (place == slots_in).astype(jnp.float32).astype(jnp.bfloat16)
    hot_out = (place == slots_out).astype(jnp.float32).astype(jnp.bfloat16)
    lane = lax.broadcasted_iota(jnp.int32, (8, 2 * mig), 1)
    first = lax.broadcasted_iota(jnp.int32, (8, 2 * mig), 0) == 0
    shift = jnp.where(first, jnp.where(lane < mig, edge[0], -edge[0]), 0.0)
    leavers = joined(
        jnp.dot(thirds(payload).astype(jnp.bfloat16), hot_out, preferred_element_type=jnp.float32)
    )
    outgoing[...] = leavers + shift

    def spread(value):
        return lax.dot_general(
            value.astype(jnp.bfloat16),
            hot_in,
            (((1,), (1,)), ((), ())),
            preferred_element_type=jnp.float32,
        )

    gone = spread(jnp.ones((8, 2 * mig), jnp.float32))

    pl.semaphore_wait(barrier, total - 1)
    moves = []
    for side, by in ((0, 1), (1, -1)):
        move = pltpu.make_async_remote_copy(
            src_ref=outgoing,
            dst_ref=incoming.at[side],
            send_sem=mig_send.at[side],
            recv_sem=mig_recv.at[side],
            device_id=device((by, 0, 0)),
            device_id_type=MESH,
        )
        move.start()
        moves.append(move)
    for move in moves:
        move.wait()
    merged = jnp.where(lane < mig, incoming[1], incoming[0])
    moved = jnp.where(gone > 0.5, joined(spread(thirds(merged))), payload)
    for r in range(5):
        own[r] = moved[r : r + 1]
    copies = []
    for k, o in enumerate(sorted(others, key=lambda o: -sum(map(abs, o)))):
        copy = pltpu.make_async_remote_copy(
            src_ref=own,
            dst_ref=ghost_ref.at[slot(o)],
            send_sem=send_sem.at[k],
            recv_sem=recv_sem.at[k],
            device_id=device(tuple(-x for x in o)),
            device_id_type=MESH,
        )
        copy.start()
        copies.append((copy, slot(o)))

    blocks = atoms // LANES
    lam = coupling_ref[0]
    own_slot = slot((0, 0, 0))
    ones = jnp.ones((8, LANES), jnp.bfloat16)
    for k in range(3):
        sums_ref[k] = jnp.zeros((8, LANES), jnp.float32)

    ahead = lax.broadcasted_iota(jnp.int32, (8, LANES), 1) - lax.broadcasted_iota(
        jnp.int32, (8, LANES), 0
    )
    lane = lax.broadcasted_iota(jnp.int32, (1, LANES), 1)
    tables = [jnp.zeros((1, LANES), jnp.float32)] * 3
    for k in range(sigma_ref.shape[0]):
        hit = lane == k
        tables = [
            jnp.where(hit, ref[k], table)
            for ref, table in zip((sigma_ref, depth_ref, charge_ref), tables)
        ]
    table = jnp.concatenate(
        [tables[0] * 0.5, jnp.sqrt(tables[1]) * 2.0, tables[2]] + [tables[2] * 0.0] * 5, axis=0
    )
    kinds = sigma_ref.shape[0]
    table_parts = thirds(table[:, :kinds]).astype(jnp.bfloat16)
    kind_row = lax.broadcasted_iota(jnp.int32, (kinds, atoms), 0).astype(jnp.float32)

    def look_up(place):
        onehot = (kind_row == ghost_ref[place, 3]).astype(jnp.float32).astype(jnp.bfloat16)
        found = joined(jnp.dot(table_parts, onehot, preferred_element_type=jnp.float32))
        rows = [ghost_ref[place, r] for r in range(3)]
        rows += [found[0:3], ghost_ref[place, 4], found[3:4]]
        whole = jnp.concatenate(rows, axis=0)
        for q in range(blocks):
            params[place * blocks + q] = whole[:, q * LANES : (q + 1) * LANES]

    look_up(own_slot)
    picks = (
        lax.broadcasted_iota(jnp.int32, (24, 7 * LANES), 0) % 8
        == lax.broadcasted_iota(jnp.int32, (24, 7 * LANES), 1) // LANES
    ).astype(jnp.float32).astype(jnp.bfloat16)
    for q in range(blocks):
        cols = thirds(params[own_slot * blocks + q]).T.astype(jnp.bfloat16)
        wide = jnp.dot(cols, picks, preferred_element_type=jnp.float32)
        for r in range(7):
            col = wide[:, r * LANES : (r + 1) * LANES]
            own_cols[q, r] = col * coulomb if r == 5 else col
    for q in range(blocks):
        for k in range(3):
            force_acc[q, k] = jnp.zeros((LANES, LANES), jnp.float32)

    for copy, place in copies:
        copy.wait()
        look_up(place)

    @pl.loop(0, blocks)
    def _(q):
        def entry(e):
            listed = listed_ref[q, 0, e]
            left = jnp.minimum(jnp.maximum(count_ref[0, 0, 0, q] - e, 0), 1)
            used = left.astype(jnp.float32)
            apart = jnp.abs(listed - (13 * blocks + q))
            self_lane = jnp.minimum(apart, 1) * (2 * LANES)
            image = lax.div(listed, blocks)
            a = lax.div(image, 9) - 1
            b = lax.rem(lax.div(image, 3), 3) - 1
            c = lax.rem(image, 3) - 1
            where_from = (
                slot_step(a, nx) * len(steps_of(ny)) + slot_step(b, ny)
            ) * len(steps_of(nz)) + slot_step(c, nz)
            other = params[where_from * blocks + lax.rem(listed, blocks)]
            rows = []
            for r in range(7):
                row = other[r : r + 1]
                if r < 3:
                    row = row + (a, b, c)[r].astype(jnp.float32) * edge[r]
                if 4 <= r < 6:
                    row = row * used
                rows.append(jnp.broadcast_to(row, (8, LANES)))
            xj, yj, zj, hj, ej, qj, pj = rows

            tot = jnp.zeros((8, LANES), jnp.float32)
            tot_p = jnp.zeros((8, LANES), jnp.float32)
            tot_k = jnp.zeros((8, LANES), jnp.float32)
            for g in range(LANES // 8):
                at = pl.ds(g * 8, 8)
                dx = own_cols[q, 0, at] - xj
                dy = own_cols[q, 1, at] - yj
                dz = own_cols[q, 2, at] - zj
                r2 = dx * dx + dy * dy + dz * dz
                sig = own_cols[q, 3, at] + hj
                s2 = sig * sig
                s6 = s2 * s2 * s2
                eps4 = own_cols[q, 4, at] * ej
                qq = own_cols[q, 5, at] * qj
                diag = ahead == self_lane + g * 8
                eps4 = jnp.where(diag, 0.0, eps4)
                qq = jnp.where(diag, 0.0, qq)
                p = jnp.maximum(own_cols[q, 6, at], pj)
                soft = soft_base + (soft_alpha * lam) * p
                weight = 1.0 - lam * p
                r4 = r2 * r2
                soft6 = s6 * soft + r4 * r2
                inv = 1.0 / soft6
                u = lax.rsqrt(soft + r2)
                ec = qq * u
                half = (0.5 * ec) * (u * u)
                t = s6 * inv
                et = eps4 * t
                tm = t - 1.0
                v = et * tm + ec
                m = et * (t + tm)
                kk = m * t + half
                fs = weight * (3.0 * (m * (r4 * inv)) + half)
                tot = tot + v
                tot_p = tot_p + p * v
                tot_k = tot_k + p * kk
                force_acc[q, 0, at] += fs * dx
                force_acc[q, 1, at] += fs * dy
                force_acc[q, 2, at] += fs * dz
            sums_ref[0] += tot
            sums_ref[1] += tot_p
            sums_ref[2] += tot_k

        width = listed_ref.shape[-1]
        unroll = 4 if width % 4 == 0 else 1

        @pl.loop(0, width // unroll)
        def _(step):
            for k in range(unroll):
                entry(step * unroll + k)

    folded = [jnp.sum(sums_ref[k], axis=0, keepdims=True) for k in range(3)]
    folded.append(jnp.zeros((5, LANES), jnp.float32))
    mine = jnp.concatenate(folded, axis=0)
    tile[...] = mine
    gathered[my_id] = mine

    def share(by):
        return pltpu.make_async_remote_copy(
            src_ref=tile,
            dst_ref=gathered.at[my_id],
            send_sem=sum_send.at[by],
            recv_sem=sum_recv.at[by],
            device_id=window_device(lax.rem(my_id + by, total)),
            device_id_type=MESH,
        )

    @pl.loop(1, total)
    def _(by):
        share(by).start()

    for q in range(blocks):
        for k in range(3):
            whole = force_acc[q, k]
            high = whole.astype(jnp.bfloat16)
            low = (whole - high.astype(jnp.float32)).astype(jnp.bfloat16)
            reduced = sum(
                lax.dot_general(
                    ones, part, (((1,), (1,)), ((), ())), preferred_element_type=jnp.float32
                )
                for part in (high, low)
            )
            force_ref[k, 0, 0, :, q * LANES : (q + 1) * LANES] = 2.0 * reduced[0:1]

    @pl.loop(1, total)
    def _(by):
        share(by).wait()

    summed = jnp.sum(gathered[...], axis=0)
    parts = [jnp.sum(summed[k : k + 1]) for k in range(3)]
    scale = 0.5 / float(atoms * total)
    energy_ref[0] = scale * (parts[0] - lam * parts[1])
    dhdl_ref[0] = -scale * (parts[1] + (0.5 * (1.0 - lam)) * parts[2])


def on_device(sizes, fraction, atom_type, perturbed, leaving, neighbours, counts,
              sigma_table, depth_table, charge_table, domain_edge, coupling):
    nx, ny, nz = sizes
    atoms = fraction.shape[-1]
    mig = leaving.shape[-1]
    slots = len(steps_of(nx)) * len(steps_of(ny)) * len(steps_of(nz))
    smem = pl.BlockSpec(memory_space=pltpu.SMEM)
    vmem = pl.BlockSpec(memory_space=pltpu.VMEM)
    f32 = jnp.float32

    def bound(kernel, *values):
        return lambda *refs: kernel(*values, *refs)

    blocks = atoms // LANES
    total = nx * ny * nz
    dma = pltpu.SemaphoreType.DMA
    return pl.pallas_call(
        bound(step_kernel, sizes),
        name="step",
        out_shape=(
            jax.ShapeDtypeStruct(fraction.shape, f32),
            jax.ShapeDtypeStruct((1,), f32),
            jax.ShapeDtypeStruct((1,), f32),
        ),
        in_specs=[smem] * 7 + [vmem] * 4,
        out_specs=(vmem, smem, smem),
        scratch_shapes=[
            pltpu.VMEM((slots, 5, 1, atoms), f32),
            pltpu.VMEM((8, 2 * mig), f32),
            pltpu.VMEM((2, 8, 2 * mig), f32),
            pltpu.VMEM((blocks, 7, LANES, LANES), f32),
            pltpu.VMEM((blocks, 3, LANES, LANES), f32),
            pltpu.VMEM((slots * blocks, 8, LANES), f32),
            pltpu.VMEM((3, 8, LANES), f32),
            pltpu.VMEM((8, LANES), f32),
            pltpu.VMEM((total, 8, LANES), f32),
            dma((2,)),
            dma((2,)),
            dma((slots,)),
            dma((slots,)),
            dma((total,)),
            dma((total,)),
        ],
        compiler_params=pltpu.CompilerParams(collective_id=0, has_side_effects=True),
    )(
        domain_edge,
        coupling,
        sigma_table,
        depth_table,
        charge_table,
        neighbours.reshape(blocks, 1, -1),
        counts,
        fraction,
        atom_type,
        perturbed,
        leaving,
    )


def solution(mesh):
    sizes = (mesh.shape["dx"], mesh.shape["dy"], mesh.shape["dz"])
    return jax.shard_map(
        lambda *arrays: on_device(sizes, *arrays),
        mesh=mesh,
        in_specs=(
            P(None, ("win", "dx"), "dy", "dz", None),
            P(("win", "dx"), "dy", "dz", None),
            P(("win", "dx"), "dy", "dz", None),
            P(("win", "dx"), "dy", "dz", None, None),
            P(("win", "dx"), "dy", "dz", None, None),
            P(("win", "dx"), "dy", "dz", None),
            P(),
            P(),
            P(),
            P(),
            P("win"),
        ),
        out_specs=(P(None, ("win", "dx"), "dy", "dz", None), P("win"), P("win")),
        check_vma=False,
    )
```
